32 devices in a mesh: chan: 4 (over x, core), slab: 8 (over z, y).
Axes of the slice: x: 2, y: 2, z: 4, core: 2. Of those that a mesh axis runs over, the one named last changes fastest.
Arguments:
- beam_images: float32 [64, 512, 4096], P('chan', 'slab'), may hold values from -24 to 24
- chan_weights: int32 [64], P('chan'), may hold values from 1 to 8
- freq_offsets: float32 [64], P('chan'), may hold values from -1 to 1
- half_widths: int32 [5], replicated, may hold values from 16 to 32, as said below
Outputs:
- smoothed: float32 [5, 512, 4096], P(None, 'slab', 'chan')
The draws below stay inside these ranges and needn't reach their ends.
Inputs may be any that keep to these rules, and one draw needn't show every extreme that they name: `half_widths`: each half-width is at least 16 and at most 32; at least one equals 32.
All inputs are finite; a program needn't handle non-finite values.
Results may differ from the reference program's by a relative error of at most 0.00008.
Values sent between devices are 32-bit elements; how exact they have to be, the bound alone decides.
A program may use at most 128 MiB of HBM per device.

```python
import jax
import jax.numpy as jnp
from jax import lax

NCHAN = 64
NCOLS = 4096
MOMENTS = 5
HW_MAX = 32
NROWS = 512


def draw_half_widths(key, part):
    first_key, second_key = jax.random.split(jax.random.fold_in(key, 17))
    values = jax.random.randint(first_key, (MOMENTS,), HW_MAX // 2, HW_MAX + 1)
    chosen = jax.random.randint(second_key, (), 0, MOMENTS)
    return jnp.where(jnp.arange(MOMENTS) == chosen, HW_MAX, values).astype(jnp.int32)


def with_ends(array, stream_key, low, largest):
    dims = array.shape
    spot = [jax.random.randint(jax.random.fold_in(stream_key, axis), (), 0, dims[axis]) for axis in range(len(dims))]
    array = array.at[tuple(spot)].set(low)
    longest = dims.index(max(dims))
    spot[longest] = (spot[longest] + 1) % dims[longest]
    return array.at[tuple(spot)].set(largest)


def block_scale(stream_key, extent, cuts, smallest, largest):
    gain, own = 1.0, jax.random.fold_in(stream_key, 6)
    for axis_at, blocks in cuts:
        heights = jnp.exp(jax.random.uniform(jax.random.fold_in(own, axis_at), (blocks,), jnp.float32, smallest / len(cuts), largest / len(cuts)))
        gain = gain * jnp.repeat(heights, extent[axis_at] // blocks).reshape([-1 if axis == axis_at else 1 for axis in range(len(extent))])
    return gain


def gaussian(own_key, extent, deviation, bound, pieces=(), dtype=jnp.bfloat16):
    result = jax.random.normal(own_key, extent, jnp.float32) * deviation
    if len(pieces) > 0:
        result = block_scale(own_key, extent, pieces, -0.22, 0.18) * result
    return jnp.clip(result, min=-bound, max=bound).astype(dtype)


def setup_inputs(seed: int = 0) -> dict:
    streams_of = jax.random.split(jax.random.key(seed), 5)
    return {
        "beam_images": gaussian(streams_of[0], (NCHAN, NROWS, NCOLS), 4.0, 24.0, ((0, 4), (1, 8)), jnp.float32),
        "chan_weights": with_ends(jax.random.randint(streams_of[1], (NCHAN,), 1, 9), jax.random.fold_in(streams_of[1], 1), 1, 8).astype(jnp.int32),
        "freq_offsets": jnp.clip(jax.random.uniform(streams_of[2], (NCHAN,), jnp.float32, -1.0, 1.0) * block_scale(streams_of[2], (NCHAN,), ((0, 4),), -0.4, 0.0), -1.0, 1.0),
        "half_widths": draw_half_widths(jax.random.fold_in(streams_of[4], 71), 0),
    }


def window_sum(values, reach, along):
    length = values.shape[along]
    widths = [(0, 0)] * values.ndim
    widths[along] = (HW_MAX + 1, HW_MAX)
    padded = jnp.pad(values, widths)
    running = jnp.cumsum(padded, axis=along)
    upper = lax.dynamic_slice_in_dim(running, (HW_MAX + 1 + reach).astype(jnp.int32), length, along)
    lower = lax.dynamic_slice_in_dim(running, (HW_MAX - reach).astype(jnp.int32), length, along)
    return upper - lower


def reference(beam_images, chan_weights, freq_offsets, half_widths):
    weight_floats = chan_weights.astype(jnp.float32)
    weight_total = jnp.sum(weight_floats)
    powers = jnp.stack([freq_offsets ** power for power in range(MOMENTS)])
    coefficients = powers * weight_floats[None, :] / weight_total
    flat = beam_images.reshape(NCHAN, NROWS * NCOLS)
    moments = jnp.dot(coefficients, flat, precision=lax.Precision.HIGHEST, preferred_element_type=jnp.float32)
    moments = moments.reshape(MOMENTS, NROWS, NCOLS)
    results = []
    for power in range(MOMENTS):
        reach = half_widths[power]
        summed = window_sum(window_sum(moments[power], reach, 0), reach, 1)
        results.append(summed / (2 * reach + 1).astype(jnp.float32))
    return jnp.stack(results)
```

```python
import functools

import jax
import jax.numpy as jnp
from jax import lax
from jax.experimental import pallas as pl
from jax.experimental.pallas import tpu as pltpu
from jax.sharding import PartitionSpec as P

MOMENTS = 5
HW_MAX = 32
LANES = 128
STEP = 2 * LANES
PARTS = 2
ROWS_AT_ONCE = 32
MESH = pl.DeviceIdType.MESH


def split(value):
    parts = []
    for _ in range(PARTS - 1):
        part = value.astype(jnp.bfloat16)
        parts.append(part)
        value = value - part.astype(jnp.float32)
    parts.append(value.astype(jnp.bfloat16))
    return parts


def kernel(
    chans, slabs,
    w_ref, f_ref, h_ref, beam_ref, out_ref,
    beams, pieces, band, row_band, sums, passed, crossed, ext, done, weights,
    load_sem, pass_send, pass_recv, cross_send, cross_recv,
    up_send, up_recv, down_send, down_recv, out_sem, w_send, w_recv,
):
    groups = chans // 2
    me = lax.axis_index("chan")
    slab = lax.axis_index("slab")
    group, core = me // 2, lax.rem(me, 2)
    local_chans, rows, all_cols = beam_ref.shape
    width = all_cols // chans
    steps = width // STEP
    tiles = width // LANES + 2
    chunks = width // LANES
    partner = group * 2 + (1 - core)
    not_first, not_last = slab > 0, slab < slabs - 1

    def block_of(slot):
        owner_group = lax.rem(group + slot // 2 + 1, groups)
        return owner_group * 2 + (1 - core if slot % 2 == 0 else core)

    def tile_col(slot, tile):
        return block_of(slot) * width + (tile - 1) * LANES

    def load(slot, tile):
        col = pl.multiple_of(tile_col(slot, tile), LANES)
        return pltpu.make_async_copy(
            beam_ref.at[:, :, pl.ds(col, LANES)], beams.at[slot, tile], load_sem.at[slot, tile]
        )

    def inside(slot, tile):
        col = tile_col(slot, tile)
        return jnp.logical_and(col >= 0, col < all_cols)

    def start_load(slot, tile):
        @pl.when(inside(slot, tile))
        def _():
            load(slot, tile).start()

    for slot in range(chans):
        @pl.loop(0, 4)
        def _(tile):
            start_load(slot, tile)

    @pl.loop(4, tiles)
    def _(tile):
        for slot in range(chans):
            start_load(slot, tile)

    barrier = pltpu.get_barrier_semaphore()
    for offset in range(1, chans):
        pl.semaphore_signal(
            barrier, inc=1, device_id={"chan": lax.rem(me + offset, chans)}, device_id_type=MESH
        )

    @pl.when(not_first)
    def _():
        pl.semaphore_signal(barrier, inc=1, device_id={"slab": slab - 1}, device_id_type=MESH)

    @pl.when(not_last)
    def _():
        pl.semaphore_signal(barrier, inc=1, device_id={"slab": slab + 1}, device_id_type=MESH)

    total = w_ref[0].astype(jnp.float32)
    for chan in range(1, local_chans):
        total = total + w_ref[chan].astype(jnp.float32)
    weights[0] = jnp.full(weights.shape[1:], total, jnp.float32)

    @pl.loop(0, MOMENTS)
    def _(k):
        reach = h_ref[k]
        for at in range(0, 2 * STEP, LANES):
            source = lax.broadcasted_iota(jnp.int32, (LANES, STEP), 0) + at
            target = lax.broadcasted_iota(jnp.int32, (LANES, STEP), 1)
            near = jnp.abs(source - LANES - target) <= reach
            band[k, at : at + LANES, :] = jnp.where(near, 1.0, 0.0).astype(jnp.bfloat16)
        span = rows + 2 * HW_MAX
        target = lax.broadcasted_iota(jnp.int32, (rows, span), 0)
        source = lax.broadcasted_iota(jnp.int32, (rows, span), 1)
        near = jnp.abs(source - HW_MAX - target) <= reach
        near = jnp.where(near, 1.0, 0.0).astype(jnp.bfloat16)
        for part in range(PARTS):
            row_band[k, :, part * span : (part + 1) * span] = near

    @pl.when(slab == 0)
    def _():
        @pl.loop(0, chunks)
        def _(i):
            ext[i, :, 0:HW_MAX, :] = jnp.zeros((MOMENTS, HW_MAX, LANES), jnp.float32)

    @pl.when(slab == slabs - 1)
    def _():
        @pl.loop(0, chunks)
        def _(i):
            ext[i, :, HW_MAX + rows :, :] = jnp.zeros((MOMENTS, HW_MAX, LANES), jnp.float32)

    pl.semaphore_wait(
        barrier, chans - 1 + not_first.astype(jnp.int32) + not_last.astype(jnp.int32)
    )

    def weight_copy(offset):
        return pltpu.make_async_remote_copy(
            src_ref=weights.at[0], dst_ref=weights.at[offset],
            send_sem=w_send.at[offset - 1], recv_sem=w_recv.at[offset - 1],
            device_id={"chan": lax.rem(me + offset, chans)}, device_id_type=MESH,
        )

    def pass_copy(hop, j):
        return pltpu.make_async_remote_copy(
            src_ref=sums.at[2 * hop, pl.ds(2 * j, 2)], dst_ref=passed.at[hop, pl.ds(2 * j, 2)],
            send_sem=pass_send.at[hop, j], recv_sem=pass_recv.at[hop, j],
            device_id={"chan": partner}, device_id_type=MESH,
        )

    def cross_copy(hop, i):
        other = lax.rem(group + hop + 1, groups) * 2 + core
        return pltpu.make_async_remote_copy(
            src_ref=sums.at[2 * hop + 1, i], dst_ref=crossed.at[hop, i],
            send_sem=cross_send.at[hop, i], recv_sem=cross_recv.at[hop, i],
            device_id={"chan": other}, device_id_type=MESH,
        )

    def up_copy(i):
        return pltpu.make_async_remote_copy(
            src_ref=ext.at[i, :, pl.ds(HW_MAX, HW_MAX)],
            dst_ref=ext.at[i, :, pl.ds(HW_MAX + rows, HW_MAX)],
            send_sem=up_send.at[i], recv_sem=up_recv.at[i],
            device_id={"slab": slab - 1}, device_id_type=MESH,
        )

    def down_copy(i):
        return pltpu.make_async_remote_copy(
            src_ref=ext.at[i, :, pl.ds(rows, HW_MAX)],
            dst_ref=ext.at[i, :, pl.ds(0, HW_MAX)],
            send_sem=down_send.at[i], recv_sem=down_recv.at[i],
            device_id={"slab": slab + 1}, device_id_type=MESH,
        )

    def out_copy(i):
        return pltpu.make_async_copy(
            done.at[i], out_ref.at[:, :, pl.ds(pl.multiple_of(i * LANES, LANES), LANES)],
            out_sem.at[i],
        )

    for offset in range(1, chans):
        weight_copy(offset).start()

    def moments_of(slot, tile):
        valid = inside(slot, tile)

        @pl.when(valid)
        def _():
            load(slot, tile).wait()

        @pl.when(jnp.logical_not(valid))
        def _():
            beams[slot, tile] = jnp.zeros(beams.shape[2:], jnp.float32)

        cols = pl.ds(pl.multiple_of(tile * LANES, LANES), LANES)

        @pl.loop(0, rows // ROWS_AT_ONCE)
        def _(part):
            first = pl.multiple_of(part * ROWS_AT_ONCE, ROWS_AT_ONCE)
            totals = [None] * MOMENTS
            for chan in range(local_chans):
                weight = w_ref[chan].astype(jnp.float32)
                offset = f_ref[chan]
                term = beams[slot, tile, chan, pl.ds(first, ROWS_AT_ONCE), :] * weight
                for k in range(MOMENTS):
                    if k > 0:
                        term = term * offset
                    totals[k] = term if chan == 0 else totals[k] + term
            for k in range(MOMENTS):
                for at, piece in enumerate(split(totals[k])):
                    pieces[slot, k, pl.ds(first + at * rows, ROWS_AT_ONCE), cols] = piece

    def columns_of(slot, j):
        wide = pl.ds(pl.multiple_of(j * STEP, STEP), 2 * STEP)

        @pl.loop(0, MOMENTS)
        def _(k):
            product = jnp.dot(
                pieces[slot, k, :, wide], band[k], preferred_element_type=jnp.float32
            )
            result = product[:rows]
            for at in range(1, PARTS):
                result = result + product[at * rows : (at + 1) * rows]
            sums[slot, 2 * j, k] = result[:, :LANES]
            sums[slot, 2 * j + 1, k] = result[:, LANES:]

    def step(j, first_tile, last_tile):
        def make(slot):
            @pl.loop(first_tile, last_tile)
            def _(tile):
                moments_of(slot, tile)

            columns_of(slot, j)

        for hop in range(groups):
            make(2 * hop)
            pass_copy(hop, j).start()
            make(2 * hop + 1)
            pass_copy(hop, j).wait_recv()
            for half in range(2):
                i = 2 * j + half
                sums[2 * hop + 1, i] = sums[2 * hop + 1, i] + passed[hop, i]
                if hop < groups - 1:
                    cross_copy(hop, i).start()

    def finish(i):
        value = sums[chans - 1, i]
        for hop in range(groups - 1):
            cross_copy(hop, i).wait_recv()
            value = value + crossed[hop, i]
        ext[i, :, HW_MAX : HW_MAX + rows, :] = value

        @pl.when(not_first)
        def _():
            up_copy(i).start()

        @pl.when(not_last)
        def _():
            down_copy(i).start()

    def rows_of(i):
        @pl.when(not_last)
        def _():
            up_copy(i).wait_recv()

        @pl.when(not_first)
        def _():
            down_copy(i).wait_recv()

        weight_total = weights[0]
        for offset in range(1, chans):
            weight_total = weight_total + weights[offset]
        for k in range(MOMENTS):
            both = jnp.concatenate(split(ext[i, k]), axis=0)
            summed = jnp.dot(row_band[k], both, preferred_element_type=jnp.float32)
            divisor = weight_total * (2 * h_ref[k] + 1).astype(jnp.float32)
            done[i, k] = summed * (1.0 / divisor)[0:1, :]
        out_copy(i).start()

    step(0, 0, 4)

    @pl.loop(1, steps - 1)
    def _(j):
        step(j, 2 * j + 2, 2 * j + 4)

    finish(0)
    step(steps - 1, 2 * steps, 2 * steps + 2)
    finish(1)
    for offset in range(1, chans):
        weight_copy(offset).wait_recv()

    @pl.loop(2, chunks)
    def _(i):
        finish(i)
        rows_of(i - 2)

    @pl.loop(chunks - 2, chunks)
    def _(i):
        rows_of(i)

    for offset in range(1, chans):
        weight_copy(offset).wait_send()

    @pl.loop(0, steps)
    def _(j):
        for hop in range(groups):
            pass_copy(hop, j).wait_send()

    @pl.loop(0, chunks)
    def _(i):
        for hop in range(groups - 1):
            cross_copy(hop, i).wait_send()

        @pl.when(not_first)
        def _():
            up_copy(i).wait_send()

        @pl.when(not_last)
        def _():
            down_copy(i).wait_send()

        out_copy(i).wait()


def body(chans, slabs, beam_images, chan_weights, freq_offsets, half_widths):
    local_chans, rows, all_cols = beam_images.shape
    width = all_cols // chans
    chunks, steps, tiles, groups = width // LANES, width // STEP, width // LANES + 2, chans // 2
    f32, b16 = jnp.float32, jnp.bfloat16
    dma = pltpu.SemaphoreType.DMA
    smem = pl.BlockSpec(memory_space=pltpu.SMEM)
    anywhere = pl.BlockSpec(memory_space=pl.ANY)
    span = rows + 2 * HW_MAX
    return pl.pallas_call(
        functools.partial(kernel, chans, slabs),
        out_shape=jax.ShapeDtypeStruct((MOMENTS, rows, width), f32),
        in_specs=[smem, smem, smem, anywhere],
        out_specs=anywhere,
        scratch_shapes=[
            pltpu.VMEM((chans, tiles, local_chans, rows, LANES), f32),
            pltpu.VMEM((chans, MOMENTS, PARTS * rows, tiles * LANES), b16),
            pltpu.VMEM((MOMENTS, 2 * STEP, STEP), b16),
            pltpu.VMEM((MOMENTS, rows, PARTS * span), b16),
            pltpu.VMEM((chans, chunks, MOMENTS, rows, LANES), f32),
            pltpu.VMEM((groups, chunks, MOMENTS, rows, LANES), f32),
            pltpu.VMEM((groups - 1, chunks, MOMENTS, rows, LANES), f32),
            pltpu.VMEM((chunks, MOMENTS, span, LANES), f32),
            pltpu.VMEM((chunks, MOMENTS, rows, LANES), f32),
            pltpu.VMEM((chans, 8, LANES), f32),
            dma((chans, tiles)),
            dma((groups, steps)),
            dma((groups, steps)),
            dma((groups - 1, chunks)),
            dma((groups - 1, chunks)),
            dma((chunks,)),
            dma((chunks,)),
            dma((chunks,)),
            dma((chunks,)),
            dma((chunks,)),
            dma((chans - 1,)),
            dma((chans - 1,)),
        ],
        compiler_params=pltpu.CompilerParams(
            collective_id=0, has_side_effects=True, vmem_limit_bytes=60 * 1024 * 1024
        ),
    )(chan_weights, freq_offsets, half_widths, beam_images)


def solution(mesh):
    placed = (P("chan", "slab", None), P("chan"), P("chan"), P())
    return jax.shard_map(
        functools.partial(body, mesh.shape["chan"], mesh.shape["slab"]),
        mesh=mesh, in_specs=placed, out_specs=P(None, "slab", "chan"), check_vma=False,
    )
```

```python
import functools

import jax
import jax.numpy as jnp
from jax import lax
from jax.experimental import pallas as pl
from jax.experimental.pallas import tpu as pltpu
from jax.sharding import PartitionSpec as P

MOMENTS = 5
HW_MAX = 32
LANES = 128
STEP = 2 * LANES
PARTS = 2
ROWS_AT_ONCE = 32
MESH = pl.DeviceIdType.MESH


def split(value):
    parts = []
    for _ in range(PARTS - 1):
        part = value.astype(jnp.bfloat16)
        parts.append(part)
        value = value - part.astype(jnp.float32)
    parts.append(value.astype(jnp.bfloat16))
    return parts


def kernel(
    chans, slabs,
    w_ref, f_ref, h_ref, beam_ref, out_ref,
    beams, pieces, band, row_band, sums, passed, crossed, ext, done, weights,
    load_sem, pass_send, pass_recv, cross_send, cross_recv,
    up_send, up_recv, down_send, down_recv, out_sem, w_send, w_recv,
):
    groups = chans // 2
    me = lax.axis_index("chan")
    slab = lax.axis_index("slab")
    group, core = me // 2, lax.rem(me, 2)
    local_chans, rows, all_cols = beam_ref.shape
    width = all_cols // chans
    steps = width // STEP
    tiles = width // LANES + 2
    chunks = width // LANES
    partner = group * 2 + (1 - core)
    not_first, not_last = slab > 0, slab < slabs - 1

    def block_of(slot):
        owner_group = lax.rem(group + slot // 2 + 1, groups)
        return owner_group * 2 + (1 - core if slot % 2 == 0 else core)

    def tile_col(slot, tile):
        return block_of(slot) * width + (tile - 1) * LANES

    def load(slot, tile):
        col = pl.multiple_of(tile_col(slot, tile), LANES)
        return pltpu.make_async_copy(
            beam_ref.at[:, :, pl.ds(col, LANES)], beams.at[slot, tile], load_sem.at[slot, tile]
        )

    def inside(slot, tile):
        col = tile_col(slot, tile)
        return jnp.logical_and(col >= 0, col < all_cols)

    def start_load(slot, tile):
        @pl.when(inside(slot, tile))
        def _():
            load(slot, tile).start()

    for slot in range(chans):
        @pl.loop(0, 4)
        def _(tile):
            start_load(slot, tile)

    @pl.loop(4, tiles)
    def _(tile):
        for slot in range(chans):
            start_load(slot, tile)

    barrier = pltpu.get_barrier_semaphore()
    for offset in range(1, chans):
        pl.semaphore_signal(
            barrier, inc=1, device_id={"chan": lax.rem(me + offset, chans)}, device_id_type=MESH
        )

    @pl.when(not_first)
    def _():
        pl.semaphore_signal(barrier, inc=1, device_id={"slab": slab - 1}, device_id_type=MESH)

    @pl.when(not_last)
    def _():
        pl.semaphore_signal(barrier, inc=1, device_id={"slab": slab + 1}, device_id_type=MESH)

    total = w_ref[0].astype(jnp.float32)
    for chan in range(1, local_chans):
        total = total + w_ref[chan].astype(jnp.float32)
    weights[0] = jnp.full(weights.shape[1:], total, jnp.float32)

    @pl.loop(0, MOMENTS)
    def _(k):
        reach = h_ref[k]
        for at in range(0, 2 * STEP, LANES):
            source = lax.broadcasted_iota(jnp.int32, (LANES, STEP), 0) + at
            target = lax.broadcasted_iota(jnp.int32, (LANES, STEP), 1)
            near = jnp.abs(source - LANES - target) <= reach
            band[k, at : at + LANES, :] = jnp.where(near, 1.0, 0.0).astype(jnp.bfloat16)
        span = rows + 2 * HW_MAX
        target = lax.broadcasted_iota(jnp.int32, (rows, span), 0)
        source = lax.broadcasted_iota(jnp.int32, (rows, span), 1)
        near = jnp.abs(source - HW_MAX - target) <= reach
        near = jnp.where(near, 1.0, 0.0).astype(jnp.bfloat16)
        for part in range(PARTS):
            row_band[k, :, part * span : (part + 1) * span] = near

    @pl.when(slab == 0)
    def _():
        @pl.loop(0, chunks)
        def _(i):
            ext[i, :, 0:HW_MAX, :] = jnp.zeros((MOMENTS, HW_MAX, LANES), jnp.float32)

    @pl.when(slab == slabs - 1)
    def _():
        @pl.loop(0, chunks)
        def _(i):
            ext[i, :, HW_MAX + rows :, :] = jnp.zeros((MOMENTS, HW_MAX, LANES), jnp.float32)

    pl.semaphore_wait(
        barrier, chans - 1 + not_first.astype(jnp.int32) + not_last.astype(jnp.int32)
    )

    def weight_copy(offset):
        return pltpu.make_async_remote_copy(
            src_ref=weights.at[0], dst_ref=weights.at[offset],
            send_sem=w_send.at[offset - 1], recv_sem=w_recv.at[offset - 1],
            device_id={"chan": lax.rem(me + offset, chans)}, device_id_type=MESH,
        )

    def pass_copy(hop, j):
        return pltpu.make_async_remote_copy(
            src_ref=sums.at[2 * hop, pl.ds(2 * j, 2)], dst_ref=passed.at[hop, pl.ds(2 * j, 2)],
            send_sem=pass_send.at[hop, j], recv_sem=pass_recv.at[hop, j],
            device_id={"chan": partner}, device_id_type=MESH,
        )

    def cross_copy(hop, i):
        other = lax.rem(group + hop + 1, groups) * 2 + core
        return pltpu.make_async_remote_copy(
            src_ref=sums.at[2 * hop + 1, i], dst_ref=crossed.at[hop, i],
            send_sem=cross_send.at[hop, i], recv_sem=cross_recv.at[hop, i],
            device_id={"chan": other}, device_id_type=MESH,
        )

    def up_copy(i):
        return pltpu.make_async_remote_copy(
            src_ref=ext.at[i, :, pl.ds(HW_MAX, HW_MAX)],
            dst_ref=ext.at[i, :, pl.ds(HW_MAX + rows, HW_MAX)],
            send_sem=up_send.at[i], recv_sem=up_recv.at[i],
            device_id={"slab": slab - 1}, device_id_type=MESH,
        )

    def down_copy(i):
        return pltpu.make_async_remote_copy(
            src_ref=ext.at[i, :, pl.ds(rows, HW_MAX)],
            dst_ref=ext.at[i, :, pl.ds(0, HW_MAX)],
            send_sem=down_send.at[i], recv_sem=down_recv.at[i],
            device_id={"slab": slab + 1}, device_id_type=MESH,
        )

    def out_copy(i):
        return pltpu.make_async_copy(
            done.at[i], out_ref.at[:, :, pl.ds(pl.multiple_of(i * LANES, LANES), LANES)],
            out_sem.at[i],
        )

    for offset in range(1, chans):
        weight_copy(offset).start()

    def moments_of(slot, tile):
        valid = inside(slot, tile)

        @pl.when(valid)
        def _():
            load(slot, tile).wait()

        @pl.when(jnp.logical_not(valid))
        def _():
            beams[slot, tile] = jnp.zeros(beams.shape[2:], jnp.float32)

        cols = pl.ds(pl.multiple_of(tile * LANES, LANES), LANES)

        @pl.loop(0, rows // ROWS_AT_ONCE)
        def _(part):
            first = pl.multiple_of(part * ROWS_AT_ONCE, ROWS_AT_ONCE)
            totals = [None] * MOMENTS
            for chan in range(local_chans):
                weight = w_ref[chan].astype(jnp.float32)
                offset = f_ref[chan]
                term = beams[slot, tile, chan, pl.ds(first, ROWS_AT_ONCE), :] * weight
                for k in range(MOMENTS):
                    if k > 0:
                        term = term * offset
                    totals[k] = term if chan == 0 else totals[k] + term
            for k in range(MOMENTS):
                for at, piece in enumerate(split(totals[k])):
                    pieces[slot, k, pl.ds(first + at * rows, ROWS_AT_ONCE), cols] = piece

    def columns_of(slot, j):
        wide = pl.ds(pl.multiple_of(j * STEP, STEP), 2 * STEP)

        for k in range(MOMENTS):
            product = jnp.dot(
                pieces[slot, k, :, wide], band[k], preferred_element_type=jnp.float32
            )
            result = product[:rows]
            for at in range(1, PARTS):
                result = result + product[at * rows : (at + 1) * rows]
            sums[slot, 2 * j, k] = result[:, :LANES]
            sums[slot, 2 * j + 1, k] = result[:, LANES:]

    def step(j, first_tile, last_tile):
        def make(slot):
            @pl.loop(first_tile, last_tile)
            def _(tile):
                moments_of(slot, tile)

            columns_of(slot, j)

        for hop in range(groups):
            make(2 * hop)
            pass_copy(hop, j).start()
            make(2 * hop + 1)
            pass_copy(hop, j).wait_recv()
            for half in range(2):
                i = 2 * j + half
                sums[2 * hop + 1, i] = sums[2 * hop + 1, i] + passed[hop, i]
                if hop < groups - 1:
                    cross_copy(hop, i).start()

    def finish(i):
        value = sums[chans - 1, i]
        for hop in range(groups - 1):
            cross_copy(hop, i).wait_recv()
            value = value + crossed[hop, i]
        ext[i, :, HW_MAX : HW_MAX + rows, :] = value

        @pl.when(not_first)
        def _():
            up_copy(i).start()

        @pl.when(not_last)
        def _():
            down_copy(i).start()

    def rows_of(i):
        @pl.when(not_last)
        def _():
            up_copy(i).wait_recv()

        @pl.when(not_first)
        def _():
            down_copy(i).wait_recv()

        weight_total = weights[0]
        for offset in range(1, chans):
            weight_total = weight_total + weights[offset]
        for k in range(MOMENTS):
            both = jnp.concatenate(split(ext[i, k]), axis=0)
            summed = jnp.dot(row_band[k], both, preferred_element_type=jnp.float32)
            divisor = weight_total * (2 * h_ref[k] + 1).astype(jnp.float32)
            done[i, k] = summed * (1.0 / divisor)[0:1, :]
        out_copy(i).start()

    step(0, 0, 4)
    for offset in range(1, chans):
        weight_copy(offset).wait_recv()

    @pl.loop(1, steps)
    def _(j):
        step(j, 2 * j + 2, 2 * j + 4)
        finish(j - 1)

    @pl.loop(steps - 1, chunks)
    def _(i):
        finish(i)

        @pl.when(i == steps - 1)
        def _():
            @pl.loop(0, steps - 3)
            def _(late):
                rows_of(late)

        rows_of(i - 2)

    @pl.loop(chunks - 2, chunks)
    def _(i):
        rows_of(i)

    for offset in range(1, chans):
        weight_copy(offset).wait_send()

    @pl.loop(0, steps)
    def _(j):
        for hop in range(groups):
            pass_copy(hop, j).wait_send()

    @pl.loop(0, chunks)
    def _(i):
        for hop in range(groups - 1):
            cross_copy(hop, i).wait_send()

        @pl.when(not_first)
        def _():
            up_copy(i).wait_send()

        @pl.when(not_last)
        def _():
            down_copy(i).wait_send()

        out_copy(i).wait()


def body(chans, slabs, beam_images, chan_weights, freq_offsets, half_widths):
    local_chans, rows, all_cols = beam_images.shape
    width = all_cols // chans
    chunks, steps, tiles, groups = width // LANES, width // STEP, width // LANES + 2, chans // 2
    f32, b16 = jnp.float32, jnp.bfloat16
    dma = pltpu.SemaphoreType.DMA
    smem = pl.BlockSpec(memory_space=pltpu.SMEM)
    anywhere = pl.BlockSpec(memory_space=pl.ANY)
    span = rows + 2 * HW_MAX
    return pl.pallas_call(
        functools.partial(kernel, chans, slabs),
        out_shape=jax.ShapeDtypeStruct((MOMENTS, rows, width), f32),
        in_specs=[smem, smem, smem, anywhere],
        out_specs=anywhere,
        scratch_shapes=[
            pltpu.VMEM((chans, tiles, local_chans, rows, LANES), f32),
            pltpu.VMEM((chans, MOMENTS, PARTS * rows, tiles * LANES), b16),
            pltpu.VMEM((MOMENTS, 2 * STEP, STEP), b16),
            pltpu.VMEM((MOMENTS, rows, PARTS * span), b16),
            pltpu.VMEM((chans, chunks, MOMENTS, rows, LANES), f32),
            pltpu.VMEM((groups, chunks, MOMENTS, rows, LANES), f32),
            pltpu.VMEM((groups - 1, chunks, MOMENTS, rows, LANES), f32),
            pltpu.VMEM((chunks, MOMENTS, span, LANES), f32),
            pltpu.VMEM((chunks, MOMENTS, rows, LANES), f32),
            pltpu.VMEM((chans, 8, LANES), f32),
            dma((chans, tiles)),
            dma((groups, steps)),
            dma((groups, steps)),
            dma((groups - 1, chunks)),
            dma((groups - 1, chunks)),
            dma((chunks,)),
            dma((chunks,)),
            dma((chunks,)),
            dma((chunks,)),
            dma((chunks,)),
            dma((chans - 1,)),
            dma((chans - 1,)),
        ],
        compiler_params=pltpu.CompilerParams(
            collective_id=0, has_side_effects=True, vmem_limit_bytes=60 * 1024 * 1024
        ),
    )(chan_weights, freq_offsets, half_widths, beam_images)


def solution(mesh):
    placed = (P("chan", "slab", None), P("chan"), P("chan"), P())
    return jax.shard_map(
        functools.partial(body, mesh.shape["chan"], mesh.shape["slab"]),
        mesh=mesh, in_specs=placed, out_specs=P(None, "slab", "chan"), check_vma=False,
    )
```

```python
import functools

import jax
import jax.numpy as jnp
from jax import lax
from jax.experimental import pallas as pl
from jax.experimental.pallas import tpu as pltpu
from jax.sharding import PartitionSpec as P

MOMENTS = 5
HW_MAX = 32
LANES = 128
STEP = 2 * LANES
PARTS = 2
ROWS_AT_ONCE = 32
MESH = pl.DeviceIdType.MESH


def split(value):
    parts = []
    for _ in range(PARTS - 1):
        part = value.astype(jnp.bfloat16)
        parts.append(part)
        value = value - part.astype(jnp.float32)
    parts.append(value.astype(jnp.bfloat16))
    return parts


def kernel(
    chans, slabs,
    w_ref, f_ref, h_ref, beam_ref, out_ref,
    beams, pieces, band, row_band, sums, passed, crossed, ext, weights,
    load_sem, pass_send, pass_recv, cross_send, cross_recv,
    up_send, up_recv, down_send, down_recv, w_send, w_recv,
):
    groups = chans // 2
    me = lax.axis_index("chan")
    slab = lax.axis_index("slab")
    group, core = me // 2, lax.rem(me, 2)
    local_chans, rows, all_cols = beam_ref.shape
    width = all_cols // chans
    steps = width // STEP
    tiles = width // LANES + 2
    chunks = width // LANES
    partner = group * 2 + (1 - core)
    not_first, not_last = slab > 0, slab < slabs - 1

    def block_of(slot):
        owner_group = lax.rem(group + slot // 2 + 1, groups)
        return owner_group * 2 + (1 - core if slot % 2 == 0 else core)

    def tile_col(slot, tile):
        return block_of(slot) * width + (tile - 1) * LANES

    def load(slot, tile):
        col = pl.multiple_of(tile_col(slot, tile), LANES)
        return pltpu.make_async_copy(
            beam_ref.at[:, :, pl.ds(col, LANES)], beams.at[slot, tile], load_sem.at[slot, tile]
        )

    def inside(slot, tile):
        col = tile_col(slot, tile)
        return jnp.logical_and(col >= 0, col < all_cols)

    def start_load(slot, tile):
        @pl.when(inside(slot, tile))
        def _():
            load(slot, tile).start()

    for slot in range(chans):
        @pl.loop(0, 4)
        def _(tile):
            start_load(slot, tile)

    @pl.loop(4, tiles)
    def _(tile):
        for slot in range(chans):
            start_load(slot, tile)

    barrier = pltpu.get_barrier_semaphore()
    for offset in range(1, chans):
        pl.semaphore_signal(
            barrier, inc=1, device_id={"chan": lax.rem(me + offset, chans)}, device_id_type=MESH
        )

    @pl.when(not_first)
    def _():
        pl.semaphore_signal(barrier, inc=1, device_id={"slab": slab - 1}, device_id_type=MESH)

    @pl.when(not_last)
    def _():
        pl.semaphore_signal(barrier, inc=1, device_id={"slab": slab + 1}, device_id_type=MESH)

    total = w_ref[0].astype(jnp.float32)
    for chan in range(1, local_chans):
        total = total + w_ref[chan].astype(jnp.float32)
    weights[0] = jnp.full(weights.shape[1:], total, jnp.float32)

    @pl.loop(0, MOMENTS)
    def _(k):
        reach = h_ref[k]
        for at in range(0, 2 * STEP, LANES):
            source = lax.broadcasted_iota(jnp.int32, (LANES, STEP), 0) + at
            target = lax.broadcasted_iota(jnp.int32, (LANES, STEP), 1)
            near = jnp.abs(source - LANES - target) <= reach
            band[k, at : at + LANES, :] = jnp.where(near, 1.0, 0.0).astype(jnp.bfloat16)
        span = rows + 2 * HW_MAX
        target = lax.broadcasted_iota(jnp.int32, (rows, span), 0)
        source = lax.broadcasted_iota(jnp.int32, (rows, span), 1)
        near = jnp.abs(source - HW_MAX - target) <= reach
        near = jnp.where(near, 1.0, 0.0).astype(jnp.bfloat16)
        for part in range(PARTS):
            row_band[k, :, part * span : (part + 1) * span] = near

    @pl.when(slab == 0)
    def _():
        @pl.loop(0, chunks)
        def _(i):
            ext[i, :, 0:HW_MAX, :] = jnp.zeros((MOMENTS, HW_MAX, LANES), jnp.float32)

    @pl.when(slab == slabs - 1)
    def _():
        @pl.loop(0, chunks)
        def _(i):
            ext[i, :, HW_MAX + rows :, :] = jnp.zeros((MOMENTS, HW_MAX, LANES), jnp.float32)

    pl.semaphore_wait(
        barrier, chans - 1 + not_first.astype(jnp.int32) + not_last.astype(jnp.int32)
    )

    def weight_copy(offset):
        return pltpu.make_async_remote_copy(
            src_ref=weights.at[0], dst_ref=weights.at[offset],
            send_sem=w_send.at[offset - 1], recv_sem=w_recv.at[offset - 1],
            device_id={"chan": lax.rem(me + offset, chans)}, device_id_type=MESH,
        )

    def pass_copy(hop, j):
        return pltpu.make_async_remote_copy(
            src_ref=sums.at[2 * hop, pl.ds(2 * j, 2)], dst_ref=passed.at[hop, pl.ds(2 * j, 2)],
            send_sem=pass_send.at[hop, j], recv_sem=pass_recv.at[hop, j],
            device_id={"chan": partner}, device_id_type=MESH,
        )

    def cross_copy(hop, i):
        other = lax.rem(group + hop + 1, groups) * 2 + core
        return pltpu.make_async_remote_copy(
            src_ref=sums.at[2 * hop + 1, i], dst_ref=crossed.at[hop, i],
            send_sem=cross_send.at[hop, i], recv_sem=cross_recv.at[hop, i],
            device_id={"chan": other}, device_id_type=MESH,
        )

    def up_copy(i):
        return pltpu.make_async_remote_copy(
            src_ref=ext.at[i, :, pl.ds(HW_MAX, HW_MAX)],
            dst_ref=ext.at[i, :, pl.ds(HW_MAX + rows, HW_MAX)],
            send_sem=up_send.at[i], recv_sem=up_recv.at[i],
            device_id={"slab": slab - 1}, device_id_type=MESH,
        )

    def down_copy(i):
        return pltpu.make_async_remote_copy(
            src_ref=ext.at[i, :, pl.ds(rows, HW_MAX)],
            dst_ref=ext.at[i, :, pl.ds(0, HW_MAX)],
            send_sem=down_send.at[i], recv_sem=down_recv.at[i],
            device_id={"slab": slab + 1}, device_id_type=MESH,
        )

    for offset in range(1, chans):
        weight_copy(offset).start()

    def moments_of(slot, tile):
        valid = inside(slot, tile)

        @pl.when(valid)
        def _():
            load(slot, tile).wait()

        @pl.when(jnp.logical_not(valid))
        def _():
            beams[slot, tile] = jnp.zeros(beams.shape[2:], jnp.float32)

        cols = pl.ds(pl.multiple_of(tile * LANES, LANES), LANES)

        @pl.loop(0, rows // ROWS_AT_ONCE)
        def _(part):
            first = pl.multiple_of(part * ROWS_AT_ONCE, ROWS_AT_ONCE)
            totals = [None] * MOMENTS
            for chan in range(local_chans):
                weight = w_ref[chan].astype(jnp.float32)
                offset = f_ref[chan]
                term = beams[slot, tile, chan, pl.ds(first, ROWS_AT_ONCE), :] * weight
                for k in range(MOMENTS):
                    if k > 0:
                        term = term * offset
                    totals[k] = term if chan == 0 else totals[k] + term
            for k in range(MOMENTS):
                for at, piece in enumerate(split(totals[k])):
                    pieces[slot, k, pl.ds(first + at * rows, ROWS_AT_ONCE), cols] = piece

    def columns_of(slot, j):
        wide = pl.ds(pl.multiple_of(j * STEP, STEP), 2 * STEP)

        for k in range(MOMENTS):
            product = jnp.dot(
                pieces[slot, k, :, wide], band[k], preferred_element_type=jnp.float32
            )
            result = product[:rows]
            for at in range(1, PARTS):
                result = result + product[at * rows : (at + 1) * rows]
            sums[slot, 2 * j, k] = result[:, :LANES]
            sums[slot, 2 * j + 1, k] = result[:, LANES:]

    def step(j, first_tile, last_tile, hops):
        def make(slot):
            @pl.loop(first_tile, last_tile)
            def _(tile):
                moments_of(slot, tile)

            columns_of(slot, j)

        for hop in hops:
            make(2 * hop)
            pass_copy(hop, j).start()
            make(2 * hop + 1)
            pass_copy(hop, j).wait_recv()
            for half in range(2):
                i = 2 * j + half
                sums[2 * hop + 1, i] = sums[2 * hop + 1, i] + passed[hop, i]
                if hop < groups - 1:
                    cross_copy(hop, i).start()

    def finish(i):
        value = sums[chans - 1, i]
        for hop in range(groups - 1):
            cross_copy(hop, i).wait_recv()
            value = value + crossed[hop, i]
        ext[i, :, HW_MAX : HW_MAX + rows, :] = value

        @pl.when(not_first)
        def _():
            up_copy(i).start()

        @pl.when(not_last)
        def _():
            down_copy(i).start()

    def rows_of(i):
        @pl.when(not_last)
        def _():
            up_copy(i).wait_recv()

        @pl.when(not_first)
        def _():
            down_copy(i).wait_recv()

        weight_total = weights[0]
        for offset in range(1, chans):
            weight_total = weight_total + weights[offset]
        for k in range(MOMENTS):
            both = jnp.concatenate(split(ext[i, k]), axis=0)
            summed = jnp.dot(row_band[k], both, preferred_element_type=jnp.float32)
            divisor = weight_total * (2 * h_ref[k] + 1).astype(jnp.float32)
            out_ref[k, :, pl.ds(pl.multiple_of(i * LANES, LANES), LANES)] = (
                summed * (1.0 / divisor)[0:1, :]
            )

    step(0, 0, 4, range(groups))

    @pl.loop(1, steps)
    def _(j):
        step(j, 2 * j + 2, 2 * j + 4, range(groups - 1))
        finish(j - 1)
        step(j, 2 * j + 2, 2 * j + 4, range(groups - 1, groups))

    for offset in range(1, chans):
        weight_copy(offset).wait_recv()

    @pl.loop(steps - 1, chunks)
    def _(i):
        finish(i)

        @pl.when(i == steps - 1)
        def _():
            @pl.loop(0, steps - 3)
            def _(late):
                rows_of(late)

        rows_of(i - 2)

    @pl.loop(chunks - 2, chunks)
    def _(i):
        rows_of(i)

    for offset in range(1, chans):
        weight_copy(offset).wait_send()

    @pl.loop(0, steps)
    def _(j):
        for hop in range(groups):
            pass_copy(hop, j).wait_send()

    @pl.loop(0, chunks)
    def _(i):
        for hop in range(groups - 1):
            cross_copy(hop, i).wait_send()

        @pl.when(not_first)
        def _():
            up_copy(i).wait_send()

        @pl.when(not_last)
        def _():
            down_copy(i).wait_send()


def body(chans, slabs, beam_images, chan_weights, freq_offsets, half_widths):
    local_chans, rows, all_cols = beam_images.shape
    width = all_cols // chans
    chunks, steps, tiles, groups = width // LANES, width // STEP, width // LANES + 2, chans // 2
    f32, b16 = jnp.float32, jnp.bfloat16
    dma = pltpu.SemaphoreType.DMA
    smem = pl.BlockSpec(memory_space=pltpu.SMEM)
    anywhere = pl.BlockSpec(memory_space=pl.ANY)
    span = rows + 2 * HW_MAX
    return pl.pallas_call(
        functools.partial(kernel, chans, slabs),
        out_shape=jax.ShapeDtypeStruct((MOMENTS, rows, width), f32),
        in_specs=[smem, smem, smem, anywhere],
        out_specs=pl.BlockSpec(memory_space=pltpu.VMEM),
        scratch_shapes=[
            pltpu.VMEM((chans, tiles, local_chans, rows, LANES), f32),
            pltpu.VMEM((chans, MOMENTS, PARTS * rows, tiles * LANES), b16),
            pltpu.VMEM((MOMENTS, 2 * STEP, STEP), b16),
            pltpu.VMEM((MOMENTS, rows, PARTS * span), b16),
            pltpu.VMEM((chans, chunks, MOMENTS, rows, LANES), f32),
            pltpu.VMEM((groups, chunks, MOMENTS, rows, LANES), f32),
            pltpu.VMEM((groups - 1, chunks, MOMENTS, rows, LANES), f32),
            pltpu.VMEM((chunks, MOMENTS, span, LANES), f32),
            pltpu.VMEM((chans, 8, LANES), f32),
            dma((chans, tiles)),
            dma((groups, steps)),
            dma((groups, steps)),
            dma((groups - 1, chunks)),
            dma((groups - 1, chunks)),
            dma((chunks,)),
            dma((chunks,)),
            dma((chunks,)),
            dma((chunks,)),
            dma((chans - 1,)),
            dma((chans - 1,)),
        ],
        compiler_params=pltpu.CompilerParams(
            collective_id=0, has_side_effects=True, vmem_limit_bytes=44 * 1024 * 1024
        ),
    )(chan_weights, freq_offsets, half_widths, beam_images)


def solution(mesh):
    placed = (P("chan", "slab", None), P("chan"), P("chan"), P())
    return jax.shard_map(
        functools.partial(body, mesh.shape["chan"], mesh.shape["slab"]),
        mesh=mesh, in_specs=placed, out_specs=P(None, "slab", "chan"), check_vma=False,
    )
```
